256 devices in a mesh: grp: 8 (over x, core), lat: 32 (over y, z).
Axes of the slice: x: 4, y: 4, z: 8, core: 2. Of those that a mesh axis runs over, the one named last changes fastest.
Arguments:
- grid_state: bfloat16 [32, 192, 384, 128], P('grp', 'lat'), may hold values from -6 to 6
- noise_field: bfloat16 [32, 192, 384, 128], P('grp', 'lat'), may hold values from -6 to 6
- legendre: bfloat16 [192, 128, 128], P('lat'), may hold values from -0.4375 to 0.4375
- diffusion: float32 [128], replicated, may hold values from 0.1 to 10
- input_weight: bfloat16 [128, 256], replicated, may hold values from -0.5 to 0.5
- noise_weight: bfloat16 [128, 256], replicated, may hold values from -0.5 to 0.5
- input_bias: float32 [256], replicated, may hold values from -4 to 4
- middle_weight: bfloat16 [256, 256], replicated, may hold values from -0.375 to 0.375
- output_weight: bfloat16 [256, 128], replicated, may hold values from -0.375 to 0.375
Outputs:
- new_state: bfloat16 [32, 192, 384, 128], P('grp', 'lat')
- ens_mean: float32 [192, 384, 128], P('lat')
- ens_var: float32 [192, 384, 128], P('lat')
The draws below stay inside these ranges and needn't reach their ends.
All inputs are finite; a program needn't handle non-finite values.
Results may differ from the reference program's by a relative error of at most 0.012.
Values may be sent and summed in bfloat16 or wider, within the bound.
No kernel may reach another device: no remote copies, remote signals or barrier semaphores. Data moves between devices by JAX's collectives and lax.ppermute only.
A program may use at most 128 MiB of HBM per device.

```python
import math
import jax
import jax.numpy as jnp
from jax import lax

CHAN = 128
NLON = 384
NLAT = 192
WAVES = 128
NOISE = 128
HIDDEN_SIZE = 256
MEMBERS = 32


def levels(key, extent, shards, low, largest):
    loudness = 1.0
    for dim, blocks in shards:
        draws = jax.random.uniform(jax.random.fold_in(jax.random.fold_in(key, 6), dim), (blocks,), jnp.float32, low / len(shards), largest / len(shards))
        loudness = loudness * jnp.repeat(jnp.exp(draws), extent[dim] // blocks).reshape((-1,) + (1,) * (len(extent) - 1 - dim))
    return loudness


def gaussian(own_key, shape, deviation, most, pieces=(), held_as=jnp.bfloat16):
    result = jax.random.normal(own_key, shape, jnp.float32) * deviation
    if len(pieces) > 0:
        result = levels(own_key, shape, pieces, -0.22, 0.18) * result
    return jnp.clip(result, min=-most, max=most).astype(held_as)


def setup_inputs(seed: int = 0) -> dict:
    arg_keys = jax.random.split(jax.random.key(seed), 10)
    grid_state = gaussian(arg_keys[0], (MEMBERS, NLAT, NLON, CHAN), 1.0, 6.0, ((0, 8), (1, 32)))
    noise_field = gaussian(arg_keys[1], (MEMBERS, NLAT, NLON, NOISE), 1.0, 6.0, ((0, 8), (1, 32)))
    legendre = gaussian(arg_keys[2], (NLAT, WAVES, WAVES), NLAT ** -0.5, 0.4375, ((0, 32),))
    diffusion = jnp.clip(jnp.exp(jax.random.uniform(arg_keys[3], (CHAN,), jnp.float32, math.log(0.1), math.log(10.0))), 0.1, 10.0)
    input_weight = gaussian(arg_keys[4], (CHAN, HIDDEN_SIZE), CHAN ** -0.5, 0.5)
    noise_weight = gaussian(arg_keys[5], (NOISE, HIDDEN_SIZE), NOISE ** -0.5, 0.5)
    input_bias = gaussian(arg_keys[6], (HIDDEN_SIZE,), 1.0, 4.0, (), jnp.float32)
    middle_weight = gaussian(arg_keys[7], (HIDDEN_SIZE, HIDDEN_SIZE), HIDDEN_SIZE ** -0.5, 0.375)
    output_weight = gaussian(arg_keys[8], (HIDDEN_SIZE, CHAN), HIDDEN_SIZE ** -0.5, 0.375)
    return {"grid_state": grid_state, "noise_field": noise_field, "legendre": legendre, "diffusion": diffusion, "input_weight": input_weight, "noise_weight": noise_weight, "input_bias": input_bias, "middle_weight": middle_weight, "output_weight": output_weight}


def wave_table(lon_count, wave_count):
    lon_ids = jnp.arange(lon_count, dtype=jnp.int32)[:, None]
    wave_ids = jnp.arange(wave_count, dtype=jnp.int32)[None, :]
    phase = (lon_ids * wave_ids % lon_count).astype(jnp.float32) * (2.0 * math.pi / lon_count)
    factor = math.sqrt(2.0 / lon_count)
    joined = jnp.concatenate([jnp.cos(phase), -jnp.sin(phase)], axis=1) * factor
    return joined.astype(jnp.bfloat16)

def damping_filter(diffusion, wave_count):
    degree = jnp.arange(wave_count, dtype=jnp.int32).astype(jnp.float32)
    ratio = degree * (degree + 1.0) / float((wave_count - 1) * wave_count)
    return 1.0 / (1.0 + diffusion[None, :] * (ratio * ratio)[:, None])

def reference(grid_state, noise_field, legendre, diffusion, input_weight, noise_weight, input_bias, middle_weight, output_weight):
    transform = wave_table(NLON, WAVES).astype(jnp.float32)
    legendre_values = legendre.astype(jnp.float32)
    wave_ids = jnp.arange(WAVES, dtype=jnp.int32)
    triangle = (wave_ids[None, :] >= wave_ids[:, None]).astype(jnp.float32)
    damping = damping_filter(diffusion, WAVES)

    def advance(pair):
        member_state, member_noise = pair
        fourier = jnp.einsum('lxc,xk->lkc', member_state.astype(jnp.float32), transform).astype(jnp.bfloat16)
        fourier = fourier.reshape(NLAT, 2, WAVES, CHAN).astype(jnp.float32)
        spectrum = jnp.einsum('lmn,lrmc->rmnc', legendre_values, fourier) * triangle[None, :, :, None]
        filtered = (spectrum * damping[None, None, :, :]).astype(jnp.bfloat16)
        grid_fourier = jnp.einsum('lmn,rmnc->lrmc', legendre_values, filtered.astype(jnp.float32)).astype(jnp.bfloat16)
        grid_fourier = grid_fourier.reshape(NLAT, 2 * WAVES, CHAN).astype(jnp.float32)
        smoothed = jnp.einsum('lkc,xk->lxc', grid_fourier, transform)
        flat_fields = smoothed.reshape(-1, CHAN)
        smoothed_in = flat_fields.astype(jnp.bfloat16)
        pre_act = jnp.dot(smoothed_in, input_weight, preferred_element_type=jnp.float32)
        pre_act = pre_act + jnp.dot(member_noise.reshape(-1, NOISE), noise_weight, preferred_element_type=jnp.float32)
        hidden_one = jax.nn.silu(pre_act + input_bias).astype(jnp.bfloat16)
        hidden_two = jax.nn.silu(jnp.dot(hidden_one, middle_weight, preferred_element_type=jnp.float32)).astype(jnp.bfloat16)
        tendency = jnp.dot(hidden_two, output_weight, preferred_element_type=jnp.float32)
        return (flat_fields + tendency).astype(jnp.bfloat16).reshape(NLAT, NLON, CHAN)
    new_state = lax.map(advance, (grid_state, noise_field))
    member_values = new_state.astype(jnp.float32)
    ens_mean = lax.optimization_barrier(jnp.mean(member_values, axis=0))
    ens_var = lax.optimization_barrier(jnp.sum(jnp.square(member_values - ens_mean), axis=0)) / (MEMBERS - 1)
    return (new_state, ens_mean, ens_var)
```

```python
import math

import jax
import jax.numpy as jnp
import numpy as np
from jax import lax
from jax.experimental import pallas as pl
from jax.experimental.pallas import tpu as pltpu
from jax.sharding import PartitionSpec as P

BF = jnp.bfloat16
F32 = jnp.float32


def wave_table(lon_count, wave_count):
    lon_ids = np.arange(lon_count)[:, None]
    wave_ids = np.arange(wave_count)[None, :]
    phase = (lon_ids * wave_ids % lon_count) * (2.0 * math.pi / lon_count)
    factor = math.sqrt(2.0 / lon_count)
    return np.concatenate([np.cos(phase), -np.sin(phase)], axis=1) * factor


def paired_table(lon_count, wave_count, owners):
    local = wave_count // owners
    table = wave_table(lon_count, wave_count).T.reshape(2, owners, 1, local, 1, lon_count)
    same = np.eye(2).reshape(1, 1, 2, 1, 2, 1)
    return (table * same).reshape(2 * wave_count * 2, 2 * lon_count)


def pair_order(wave_count, owners):
    local = wave_count // owners
    eye = np.eye(wave_count).reshape(owners, 1, local, 1, wave_count)
    same = np.eye(2).reshape(1, 2, 1, 2, 1)
    return (eye * same).reshape(2 * wave_count, 2 * wave_count)


def forward_kernel(grid_ref, legendre_ref, table_ref, order_ref, out_ref):
    owners, rows, _ = out_ref.shape
    half = pl.program_id(1)
    lon = grid_ref.shape[2]
    chan = grid_ref.shape[3]
    fields = jnp.concatenate(
        [grid_ref[0].reshape(2 * lon, chan), grid_ref[1].reshape(2 * lon, chan)], axis=1
    )
    coeffs = jnp.dot(table_ref[...], fields, preferred_element_type=F32).astype(BF)
    waves = coeffs.shape[0] // 2
    width = 2 * chan
    base = pl.multiple_of(half * (2 * width), 2 * width)
    out_ref[:, :, pl.ds(base, width)] = coeffs[:waves].reshape(owners, rows, width)
    out_ref[:, :, pl.ds(base + width, width)] = coeffs[waves:].reshape(owners, rows, width)

    @pl.when(half == 0)
    def _():
        basis = legendre_ref[...].reshape(-1, legendre_ref.shape[2])
        moved = jnp.dot(order_ref[...], basis, preferred_element_type=F32).astype(BF)
        out_ref[:, :, 4 * width :] = moved.reshape(owners, rows, legendre_ref.shape[2])


def spectral_kernel(first_ref, in_ref, basis_ref, diffusion_ref, out_ref, table_ref, damp_ref):
    owners, rows, width = in_ref.shape
    total = basis_ref.shape[2]
    local = table_ref.shape[1] // total

    @pl.when(pl.program_id(0) == 0)
    def _():
        basis = basis_ref[...].reshape(owners * rows, total)
        row_ids = lax.broadcasted_iota(jnp.int32, basis.shape, 0) % local
        total_ids = lax.broadcasted_iota(jnp.int32, basis.shape, 1)
        for m in range(local):
            keep = (row_ids == m) & (total_ids >= first_ref[0] + m)
            table_ref[:, m * total : (m + 1) * total] = jnp.where(keep, basis, jnp.zeros_like(basis))
        degree = lax.broadcasted_iota(jnp.int32, damp_ref.shape, 0).astype(F32)
        ratio = degree * (degree + 1.0) / float((total - 1) * total)
        damp_ref[...] = 1.0 / (1.0 + diffusion_ref[...] * (ratio * ratio))

    values = in_ref[...].reshape(owners * rows, width)
    table = table_ref[...]
    spectrum = lax.dot_general(
        table, values, (((0,), (0,)), ((), ())), preferred_element_type=F32
    )
    damping = damp_ref[...]
    chan = damping.shape[1]
    columns = [
        jnp.concatenate(
            [
                (spectrum[m * total : (m + 1) * total, k * chan : (k + 1) * chan] * damping).astype(BF)
                for m in range(local)
            ],
            axis=0,
        )
        for k in range(width // chan)
    ]
    filtered = jnp.concatenate(columns, axis=1)
    back = jnp.dot(table, filtered, preferred_element_type=F32).astype(BF)
    out_ref[...] = back.reshape(owners, rows, width)


def silu(v):
    u = 0.5 * v
    return u + u * jnp.tanh(u)


def column_kernel(
    core_ref,
    in_ref,
    noise_ref,
    table_ref,
    first_weight_ref,
    bias_ref,
    middle_ref,
    output_ref,
    state_ref,
    keep_ref,
    send_ref,
    sum_ref,
    dev_ref,
    moment_ref,
):
    owners, rows, width = in_ref.shape
    lon = noise_ref.shape[2]
    chan = noise_ref.shape[3]
    half = pl.program_id(1)
    coeffs = in_ref[...].reshape(owners * rows, width)
    stacked = jnp.concatenate([coeffs[:, : width // 2], coeffs[:, width // 2 :]], axis=0)
    smoothed = jnp.dot(table_ref[...], stacked, preferred_element_type=F32)
    values = []
    for b in range(2):
        fields = smoothed[:, b * chan : (b + 1) * chan]
        noise = noise_ref[b].reshape(2 * lon, chan)
        joined = jnp.concatenate([fields.astype(BF), noise], axis=1)
        hidden = silu(
            jnp.dot(joined, first_weight_ref[...], preferred_element_type=F32) + bias_ref[...]
        ).astype(BF)
        hidden = silu(jnp.dot(hidden, middle_ref[...], preferred_element_type=F32)).astype(BF)
        tendency = jnp.dot(hidden, output_ref[...], preferred_element_type=F32)
        state = (fields + tendency).astype(BF)
        state_ref[b] = state.reshape(2, lon, chan)
        values.append(state.astype(F32))
    pair_sum = values[0] + values[1]
    gap = values[0] - values[1]
    pair_dev = 0.5 * (gap * gap)

    @pl.when(half == 0)
    def _():
        sum_ref[...] = pair_sum
        dev_ref[...] = pair_dev

    @pl.when(half == 1)
    def _():
        other = sum_ref[...]
        total = (pair_sum + other).astype(BF)
        change = pair_sum - other
        dev = (pair_dev + dev_ref[...] + 0.25 * (change * change)).astype(BF)
        parts = keep_ref.shape[0]
        piece = keep_ref.shape[3]
        for l in range(2):
            for h in range(2):
                for q in range(parts):
                    at = l * lon + (h * parts + q) * piece
                    moment_ref[h, q, 0, l] = total[at : at + piece]
                    moment_ref[h, q, 1, l] = dev[at : at + piece]
        keep_ref[...] = moment_ref[core_ref[0]]
        send_ref[...] = moment_ref[1 - core_ref[0]]


def per_device(
    grid_state,
    noise_field,
    legendre,
    diffusion,
    input_weight,
    noise_weight,
    input_bias,
    middle_weight,
    output_weight,
):
    members, lat_rows, lon, chan = grid_state.shape
    waves, total = legendre.shape[1:]
    owners = lax.axis_size("lat")
    groups = lax.axis_size("grp")
    chips = groups // 2
    local = waves // owners
    pairs = lat_rows // 2
    rows = 2 * local
    hidden = middle_weight.shape[0]
    lanes = members * 2 * chan
    table = jnp.asarray(paired_table(lon, waves, owners), dtype=BF)
    back_table = jnp.asarray(paired_table(lon, waves, owners).T, dtype=BF)
    order = jnp.asarray(pair_order(waves, owners), dtype=BF)
    whole = lambda *shape: pl.BlockSpec(shape, lambda *_: (0,) * len(shape))
    scalar = pl.BlockSpec(memory_space=pltpu.SMEM)

    outgoing = pl.pallas_call(
        forward_kernel,
        grid=(pairs, members // 2),
        in_specs=[
            pl.BlockSpec((2, 2, lon, chan), lambda p, h: (h, p, 0, 0)),
            pl.BlockSpec((2, waves, total), lambda p, h: (p, 0, 0)),
            whole(*table.shape),
            whole(*order.shape),
        ],
        out_specs=pl.BlockSpec((owners, rows, lanes + total), lambda p, h: (0, p, 0)),
        out_shape=jax.ShapeDtypeStruct((owners, pairs * rows, lanes + total), BF),
        name="forward",
    )(grid_state, legendre, table, order)
    incoming = lax.all_to_all(outgoing, "lat", 0, 0, tiled=True)

    first = (lax.axis_index("lat") * local).astype(jnp.int32).reshape(1)
    width = 2 * chan
    banded = pl.pallas_call(
        spectral_kernel,
        grid=(lanes // width,),
        in_specs=[
            scalar,
            pl.BlockSpec((owners, pairs * rows, width), lambda i: (0, 0, i)),
            pl.BlockSpec((owners, pairs * rows, total), lambda i: (0, 0, lanes // total)),
            whole(1, chan),
        ],
        out_specs=pl.BlockSpec((owners, pairs * rows, width), lambda i: (0, 0, i)),
        out_shape=jax.ShapeDtypeStruct((owners, pairs * rows, lanes), BF),
        scratch_shapes=[
            pltpu.VMEM((owners * pairs * rows, local * total), BF),
            pltpu.VMEM((total, chan), F32),
        ],
        name="spectral",
    )(first, incoming, incoming, diffusion.reshape(1, chan))
    returned = lax.all_to_all(banded, "lat", 0, 0, tiled=True)

    core = (lax.axis_index("grp") % 2).astype(jnp.int32).reshape(1)
    first_weight = jnp.concatenate([input_weight, noise_weight], axis=0)
    piece = lon // (2 * chips)
    moment_shape = (chips, 2, lat_rows, piece, chan)
    moment_block = (chips, 2, 2, piece, chan)
    moment_spec = pl.BlockSpec(moment_block, lambda p, h: (0, 0, p, 0, 0))
    new_state, keep, send = pl.pallas_call(
        column_kernel,
        grid=(pairs, members // 2),
        in_specs=[
            scalar,
            pl.BlockSpec((owners, rows, 4 * chan), lambda p, h: (0, p, h)),
            pl.BlockSpec((2, 2, lon, chan), lambda p, h: (h, p, 0, 0)),
            whole(*back_table.shape),
            whole(2 * chan, hidden),
            whole(1, hidden),
            whole(hidden, hidden),
            whole(hidden, chan),
        ],
        out_specs=[
            pl.BlockSpec((2, 2, lon, chan), lambda p, h: (h, p, 0, 0)),
            moment_spec,
            moment_spec,
        ],
        out_shape=[
            jax.ShapeDtypeStruct(grid_state.shape, BF),
            jax.ShapeDtypeStruct(moment_shape, BF),
            jax.ShapeDtypeStruct(moment_shape, BF),
        ],
        scratch_shapes=[
            pltpu.VMEM((2 * lon, chan), F32),
            pltpu.VMEM((2 * lon, chan), F32),
            pltpu.VMEM((2,) + moment_block, BF),
        ],
        name="column",
    )(
        core,
        returned,
        noise_field,
        back_table,
        first_weight,
        input_bias.reshape(1, hidden),
        middle_weight,
        output_weight,
    )

    swap = [(i, i ^ 1) for i in range(groups)]
    lines = [list(range(k, groups, 2)) for k in range(2)]
    got = lax.ppermute(send, "grp", swap).astype(F32)
    kept = keep.astype(F32)
    change = kept[:, 0] - got[:, 0]
    chip_sum = kept[:, 0] + got[:, 0]
    chip_members = 2 * members
    chip_dev = kept[:, 1] + got[:, 1] + change * change / chip_members
    chip_moments = jnp.stack([chip_sum, chip_dev], axis=1).astype(BF)
    gathered = lax.all_to_all(
        chip_moments, "grp", 0, 0, tiled=True, axis_index_groups=lines
    ).astype(F32)
    sums = gathered[:, 0]
    whole_sum = sums.sum(0)
    shift = sums - (whole_sum / chips)[None]
    devs = gathered[:, 1].sum(0) + (shift * shift).sum(0) / chip_members
    ensemble = members * groups
    result = jnp.stack([whole_sum / ensemble, devs / (ensemble - 1)]).astype(BF)
    mine = lax.all_gather(result, "grp", axis=0, axis_index_groups=lines)
    other = lax.ppermute(mine, "grp", swap)
    low = jnp.where(core[0] == 0, mine, other)
    high = jnp.where(core[0] == 0, other, mine)
    both = jnp.stack([low, high])
    out = both.transpose(2, 3, 0, 1, 4, 5).reshape(2, lat_rows, lon, chan).astype(F32)
    return (new_state, out[0], out[1])


def solution(mesh):
    in_specs = (
        P("grp", "lat", None, None),
        P("grp", "lat", None, None),
        P("lat", None, None),
        P(),
        P(),
        P(),
        P(),
        P(),
        P(),
    )
    out_specs = (P("grp", "lat", None, None), P("lat", None, None), P("lat", None, None))
    return jax.shard_map(
        per_device, mesh=mesh, in_specs=in_specs, out_specs=out_specs, check_vma=False
    )
```
